256 devices in a mesh: chrom: 2 (over y), var: 128 (over z, x, core).
Axes of the slice: x: 4, y: 2, z: 16, core: 2. Of those that a mesh axis runs over, the one named last changes fastest.
The devices are a block of a 4x16x16 slice.
Arguments:
- genotypes: bfloat16 [2048, 131072], P(None, ('chrom', 'var')), parts along dimension 1, may hold values from -6 to 6
- weights: float32 [4096, 32, 3072], P(('chrom', 'var')), parts along dimension 0, may hold values from -0.109375 to 0.109375
- starts: int32 [4096], P(('chrom', 'var')), parts along dimension 0, may hold values from 0 to 65535, as said below
- ends: int32 [4096], P(('chrom', 'var')), parts along dimension 0, may hold values from 1 to 65536, as said below
- phenotypes: float32 [2048, 32], replicated, may hold values from -6 to 6
Outputs:
- scores: float32 [4096, 1024], P(('chrom', 'var')), parts along dimension 0
- linkage: bfloat16 [131072, 1536], P(('chrom', 'var')), parts along dimension 0
The draws below stay inside these ranges and needn't reach their ends.
There are 2 independent parts, one for each index of `chrom`. The reference program is written for one: setup_inputs(seed, part) draws one part's arguments, and reference() takes and returns one part's arrays. A program takes and returns all parts, laid end to end along the dimension named above; an argument that names none is the same for every part. Nothing has to cross between parts.
Inputs may be any that keep to these rules, and one draw needn't show every extreme that they name: starts[g] lies between (g // 16) * 512 and (g // 16) * 512 + 511. ends[g] - starts[g] is between 1 and 3072, equals 3072 for gene 0, and ends[g] <= 65536.
All inputs are finite; a program needn't handle non-finite values.
Results may differ from the reference program's by a relative error of at most 0.0057.
Values may be sent and summed in bfloat16 or wider, within the bound.
No kernel may reach another device: no remote copies, remote signals or barrier semaphores. Data moves between devices by JAX's collectives and lax.ppermute only.
A program may use at most 128 MiB of HBM per device.

```python
import jax
import jax.numpy as jnp
from jax import lax

SAMPLES = 2048
VB = 512
V = 65536
GENE_DEV = 16
GENES = 2048
TISSUES = 32
PHENO = 32
WMAX = 3072
WMIN = 1024
REACH = 6


def draw_genotypes(key, part):
    noise = jax.random.normal(jax.random.fold_in(key, 11), (SAMPLES, V), jnp.float32)
    return jnp.clip(noise, -6.0, 6.0).astype(jnp.bfloat16)


def window_bounds(key):
    base = jax.random.fold_in(key, 5)
    gene_index = jnp.arange(GENES, dtype=jnp.int32)
    block_index = gene_index // GENE_DEV
    offsets = jax.random.randint(jax.random.fold_in(base, 1), (GENES,), 0, VB, jnp.int32)
    lengths = jax.random.randint(jax.random.fold_in(base, 2), (GENES,), WMIN, WMAX + 1, jnp.int32)
    lengths = jnp.where(gene_index % GENE_DEV == 0, WMAX, lengths)
    first = block_index * VB + offsets
    last = jnp.minimum(first + lengths, V)
    return (first.astype(jnp.int32), last.astype(jnp.int32))


def draw_starts(key, part):
    return window_bounds(key)[0]


def draw_ends(key, part):
    return window_bounds(key)[1]


def levels(stream_key, shape, cuts, least, high):
    gain = 1.0
    for dim, shards_of in cuts:
        draws = jax.random.uniform(jax.random.fold_in(jax.random.fold_in(stream_key, 6), dim), (shards_of,), jnp.float32, least / len(cuts), high / len(cuts))
        gain = gain * jnp.repeat(jnp.exp(draws), shape[dim] // shards_of).reshape((-1,) + (1,) * (len(shape) - 1 - dim))
    return gain


def normal_values(own_key, shape, scale, most, pieces=(), kind=jnp.bfloat16):
    drawn = jax.random.normal(own_key, shape, jnp.float32) * scale
    if len(pieces) > 0:
        drawn = levels(own_key, shape, pieces, -0.22, 0.18) * drawn
    return jnp.clip(drawn, min=-most, max=most).astype(kind)


def setup_inputs(seed: int = 0, part: int = 0) -> dict:
    arg_keys = jax.random.split(jax.random.key(seed), 6)
    part_splits = jax.random.split(jax.random.fold_in(arg_keys[5], part), 6)
    return {
        "genotypes": draw_genotypes(jax.random.fold_in(jax.random.fold_in(arg_keys[5], part), 71), part),
        "weights": normal_values(part_splits[1], (GENES, TISSUES, WMAX), WMAX ** -0.5, 0.109375, ((0, 128),), jnp.float32),
        "starts": draw_starts(jax.random.fold_in(jax.random.fold_in(arg_keys[5], part), 71), part),
        "ends": draw_ends(jax.random.fold_in(jax.random.fold_in(arg_keys[5], part), 71), part),
        "phenotypes": normal_values(arg_keys[4], (SAMPLES, PHENO), 1.0, 6.0, (), jnp.float32),
    }


EPSILON = 1e-05

def standardize(values):
    centre = lax.optimization_barrier(jnp.mean(values, axis=0))
    centred = values - centre
    spread = lax.optimization_barrier(jnp.mean(centred * centred, axis=0))
    return (centred * lax.rsqrt(spread + EPSILON)).astype(jnp.bfloat16)

def place_weights(gene_weights, gene_starts, gene_ends, anchor, window_cols):
    span = gene_weights.shape[2]
    column = jnp.arange(span, dtype=jnp.int32)
    lengths = (gene_ends - gene_starts).astype(jnp.int32)
    rounded = gene_weights.astype(jnp.bfloat16)
    masked = jnp.where(column[None, None, :] < lengths[:, None, None], rounded, jnp.zeros_like(rounded))
    padded = jnp.pad(masked, ((0, 0), (0, 0), (window_cols, window_cols - span)))
    offsets = (gene_starts - anchor).astype(jnp.int32)

    def place_one(single, offset):
        return lax.dynamic_slice_in_dim(single, (window_cols - offset).astype(jnp.int32), window_cols, 1)
    placed = jax.vmap(place_one)(padded, offsets)
    return placed.reshape(-1, window_cols)

def reference(genotypes, weights, starts, ends, phenotypes):
    window_cols = (REACH + 1) * VB
    blocks = GENES // GENE_DEV
    gene_cols = GENE_DEV * TISSUES
    padded = jnp.concatenate([genotypes, jnp.zeros((SAMPLES, REACH * VB), genotypes.dtype)], axis=1)

    def one_block(block_index):
        region = lax.dynamic_slice_in_dim(padded, (block_index * VB).astype(jnp.int32), window_cols, 1)
        first_gene = (block_index * GENE_DEV).astype(jnp.int32)
        own_weights = lax.dynamic_slice_in_dim(weights, first_gene, GENE_DEV, 0)
        own_starts = lax.dynamic_slice_in_dim(starts, first_gene, GENE_DEV, 0)
        own_ends = lax.dynamic_slice_in_dim(ends, first_gene, GENE_DEV, 0)
        placed = place_weights(own_weights, own_starts, own_ends, (block_index * VB).astype(jnp.int32), window_cols)
        return jnp.dot(region, placed.T, preferred_element_type=jnp.float32)
    expression = lax.map(one_block, jnp.arange(blocks, dtype=jnp.int32))
    expression = jnp.transpose(expression, (1, 0, 2)).reshape(SAMPLES, GENES * TISSUES)
    scaled = standardize(expression)
    pheno_scaled = standardize(phenotypes)
    scores = jnp.dot(scaled.T, pheno_scaled, preferred_element_type=jnp.float32) / jnp.sqrt(jnp.float32(SAMPLES))
    scores = scores.reshape(GENES, TISSUES * PHENO)
    bordered = jnp.pad(scaled, ((0, 0), (gene_cols, gene_cols)))

    def one_link(block_index):
        own_cols = lax.dynamic_slice_in_dim(scaled, (block_index * gene_cols).astype(jnp.int32), gene_cols, 1)
        beside_all = lax.dynamic_slice_in_dim(bordered, (block_index * gene_cols).astype(jnp.int32), 3 * gene_cols, 1)
        product = jnp.dot(own_cols.T, beside_all, preferred_element_type=jnp.float32)
        return (product / jnp.float32(SAMPLES)).astype(jnp.bfloat16)
    linkage = lax.map(one_link, jnp.arange(blocks, dtype=jnp.int32)).reshape(GENES * TISSUES, 3 * gene_cols)
    return (scores, linkage)
```

```python
import functools

import jax
import jax.numpy as jnp
from jax import lax
from jax.experimental import pallas as pl
from jax.experimental.pallas import tpu as pltpu
from jax.sharding import PartitionSpec as P

EPSILON = 1e-05
CORES = 2
ROW = 4


def routes(count):
    chips = count // CORES
    width = ROW if chips % ROW == 0 else 1
    rows = chips // width

    def pos(row, col, core):
        return (row * width + col) * CORES + core

    every = [(r, c, k) for r in range(rows) for c in range(width) for k in range(CORES)]
    last = width - 1
    return {
        "left": [(pos(r, c, k), pos(r, (c - 1) % width, k)) for r, c, k in every],
        "down": [(pos(r, last, k), pos(r - 1, last, k)) for r, c, k in every if c == last and r > 0],
        "far": [(i, (i - 3 * CORES) % count) for i in range(2 * CORES, count)],
        "prev": [(i, i - CORES) for i in range(CORES, count)],
        "next": [(i, (i + CORES) % count) for i in range(count)],
        "swap": [(i, i ^ 1) for i in range(count)],
        "edge": [(i, i + 1) for i in range(1, count - 1, 2)] + [(i + 1, i) for i in range(1, count - 1, 2)],
    }


def place_kernel(slab_ref, starts_ref, lengths_ref, weights_ref, out_ref, *, block_cols, anchor_cols):
    gene = pl.program_id(0)
    tissues, span = weights_ref.shape[1:]
    slabs = out_ref.shape[0]
    window = slabs * block_cols
    offset = starts_ref[gene]
    length = lengths_ref[gene]
    column = lax.broadcasted_iota(jnp.int32, (tissues, span), 1)
    values = jnp.where(column < length, weights_ref[0], 0.0)
    padded = jnp.concatenate([values, jnp.zeros((tissues, window - span), jnp.float32)], axis=1)
    rolled = pltpu.roll(padded, offset, 1).astype(jnp.bfloat16)
    for slab in range(slabs):
        out_ref[slab_ref[slab]] = rolled[:, slab * block_cols : (slab + 1) * block_cols]


def place_weights(weights, offsets, lengths, slab_order, block_cols, slabs):
    genes, tissues, span = weights.shape
    return pl.pallas_call(
        functools.partial(place_kernel, block_cols=block_cols, anchor_cols=0),
        grid_spec=pltpu.PrefetchScalarGridSpec(
            num_scalar_prefetch=3,
            grid=(genes,),
            in_specs=[pl.BlockSpec((1, tissues, span), lambda g, *_: (g, 0, 0))],
            out_specs=pl.BlockSpec((slabs, tissues, block_cols), lambda g, *_: (0, g, 0)),
        ),
        out_shape=jax.ShapeDtypeStruct((slabs, genes * tissues, block_cols), jnp.bfloat16),
        name="place",
        compiler_params=pltpu.CompilerParams(vmem_limit_bytes=16 * 1024 * 1024),
    )(slab_order, offsets, lengths, weights)


def standardize(values):
    centre = jnp.mean(values, axis=0)
    centred = values - centre
    spread = jnp.mean(centred * centred, axis=0)
    return (centred * lax.rsqrt(spread + EPSILON)).astype(jnp.bfloat16)


def cross_product(left, right):
    return lax.dot_general(
        left, right, (((0,), (0,)), ((), ())), preferred_element_type=jnp.float32
    )


def times(block, slab):
    return lax.dot_general(
        block, slab, (((1,), (1,)), ((), ())), preferred_element_type=jnp.float32
    )


def on_device(genotypes, weights, starts, ends, phenotypes):
    samples, block_cols = genotypes.shape
    reach_blocks = weights.shape[2] // block_cols
    slabs = reach_blocks + 1
    count = lax.axis_size("var")
    here = lax.axis_index("var")
    core = here % CORES
    col = (here // CORES) % ROW
    route = routes(count)

    def send(value, name):
        return lax.ppermute(value, "var", route[name])

    half = samples // 2
    own = [genotypes[:half], genotypes[half:]]
    near = [send(own[0], "left"), None]
    far = [None, send(own[1], "far")]
    near[1] = send(own[1], "left")
    far[0] = send(own[0], "far")
    near = [jnp.where(col == ROW - 1, send(value, "down"), value) for value in near]
    middle = [send(near[0], "prev"), send(far[1], "next")]
    near_beside = [send(value, "swap") for value in near]
    mixed = [send(jnp.where(core == 1, mine, other), "swap") for mine, other in zip(own, far)]
    middle_beside = [send(value, "swap") for value in middle]

    order = jnp.where(
        core == 0,
        jnp.array([0, 1, 2, 3, 4, 5, 6], jnp.int32),
        jnp.array([0, 3, 2, 5, 4, 1, 6], jnp.int32),
    )
    placed = place_weights(
        weights, starts - here * block_cols, ends - starts, order, block_cols, slabs
    )
    parts = []
    for h in range(2):
        blocks = [own[h], mixed[h], near[h], near_beside[h], middle[h], middle_beside[h], far[h]]
        total = None
        for at in (0, 2, 6, 1, 3, 4, 5):
            product = times(blocks[at], placed[at])
            total = product if total is None else total + product
        parts.append(total)
    expression = jnp.concatenate(parts, axis=0)
    scaled = standardize(expression)
    beside = send(scaled, "swap")
    edge = send(scaled, "edge")
    pheno_scaled = standardize(phenotypes)
    scores = cross_product(scaled, pheno_scaled) / jnp.sqrt(jnp.float32(samples))
    scores = scores.reshape(weights.shape[0], -1)

    def link(other):
        return (cross_product(scaled, other) / jnp.float32(samples)).astype(jnp.bfloat16)

    mine, inner, outer = link(scaled), link(beside), link(edge)
    linkage = jnp.concatenate(
        [jnp.where(core == 0, outer, inner), mine, jnp.where(core == 0, inner, outer)], axis=1
    )
    return (scores, linkage)


def solution(mesh):
    placed = (
        P(None, ("chrom", "var")),
        P(("chrom", "var"), None, None),
        P(("chrom", "var")),
        P(("chrom", "var")),
        P(),
    )
    return jax.shard_map(
        on_device,
        mesh=mesh,
        in_specs=placed,
        out_specs=(P(("chrom", "var"), None), P(("chrom", "var"), None)),
        check_vma=False,
    )
```
